32 devices in a mesh: rep: 4 (over y, x), shard: 8 (over z, core).
Axes of the slice: x: 2, y: 2, z: 4, core: 2. Of those that a mesh axis runs over, the one named last changes fastest.
Arguments:
- hot_ids: int32 [65536], P(('rep', 'shard')), may hold values from 0 to 8191
- hot_grads: bfloat16 [65536, 128], P(('rep', 'shard')), may hold values from -6 to 6
- hot_rows: float32 [8192, 128], replicated, may hold values from -6 to 6
- hot_accum: float32 [8192], replicated, may hold values from 0.5 to 4
- cold_counts: int32 [32, 32], P(('rep', 'shard')), may hold values from 1 to 16, as said below
- cold_slots: int32 [32, 32, 16], P(('rep', 'shard')), may hold values from 0 to 8191
- cold_grads: bfloat16 [32, 32, 16, 128], P(('rep', 'shard')), may hold values from -6 to 6
- cold_rows: float32 [262144, 128], P(('rep', 'shard')), may hold values from -6 to 6
- cold_accum: float32 [262144], P(('rep', 'shard')), may hold values from 0.5 to 4
Outputs:
- new_hot_rows: float32 [8192, 128], replicated
- new_hot_accum: float32 [8192], replicated
- new_cold_rows: float32 [262144, 128], P(('rep', 'shard'))
- new_cold_accum: float32 [262144], P(('rep', 'shard'))
The draws below stay inside these ranges and needn't reach their ends.
Inputs may be any that keep to these rules, and one draw needn't show every extreme that they name: `cold_counts`: every entry is at least 1 and at most 16; in every draw some owner receives 16 live slots from every sender.
All inputs are finite; a program needn't handle non-finite values.
Results may differ from the reference program's by a relative error of at most 0.0003.
Values may be sent and summed in bfloat16 or wider, within the bound.
A program may use at most 128 MiB of HBM per device.

```python
import math
import jax
import jax.numpy as jnp
import numpy as np
from jax import lax

D = 128
HOT = 8192
COLD_DEV = 8192
CAP = 16
OWNERS = 32
COLD = 262144
LOOKUPS = 65536


def draw_cold_counts(key, part):
    level_key = jax.random.fold_in(key, 11)
    draw_key = jax.random.fold_in(key, 12)
    full_key = jax.random.fold_in(key, 13)
    load_level = jax.random.randint(level_key, (OWNERS,), 1, 5)
    raw_draw = jax.random.randint(draw_key, (OWNERS, OWNERS), 0, CAP)
    counts = jnp.minimum(CAP, 1 + raw_draw * load_level[None, :] // 4)
    full_owner = jax.random.randint(full_key, (), 0, OWNERS)
    counts = jnp.where(jnp.arange(OWNERS)[None, :] == full_owner, CAP, counts)
    return counts.astype(jnp.int32)


def set_ends(array, rng, least, high):
    spot = [jax.random.randint(jax.random.fold_in(rng, axis), (), 0, length) for axis, length in enumerate(array.shape)]
    main_axis = array.shape.index(max(array.shape))
    neighbour = spot[:main_axis] + [(spot[main_axis] + 1) % array.shape[main_axis]] + spot[main_axis + 1:]
    return array.at[tuple(spot)].set(least).at[tuple(neighbour)].set(high)


def level_of(own_key, extent, cuts, least, top_value):
    def one(dim, shards_of):
        heights = jax.random.uniform(jax.random.fold_in(jax.random.fold_in(own_key, 6), dim), (shards_of,), jnp.float32, least / len(cuts), top_value / len(cuts))
        return jnp.repeat(jnp.exp(heights), extent[dim] // shards_of).reshape((-1,) + (1,) * (len(extent) - dim - 1))

    factor_of = one(*cuts[0])
    for cut in cuts[1:]:
        factor_of = factor_of * one(*cut)
    return factor_of


def rank_table(number_of, slope):
    portions = [(1 << 20) // math.isqrt(grade ** slope) + 1 for grade in range(1, number_of + 1)]
    spread = 1 + sum(portions) // (1 << 30)
    return np.cumsum(np.array([max(1, weight // spread) for weight in portions]))


def ranked_ids(key, shape, number_of, lean):
    table = rank_table(number_of, lean)
    pick = jax.random.randint(jax.random.fold_in(key, 1), shape, 0, int(table[number_of - 1]))
    grade = jnp.searchsorted(jnp.asarray(table, jnp.int32), pick, side="right")
    return jax.random.permutation(jax.random.fold_in(key, 2), number_of)[grade].astype(jnp.int32)


def noise(rng, extent, deviation, reach, shards=(), kind=jnp.bfloat16):
    result = jax.random.normal(rng, extent, jnp.float32) * deviation
    if len(shards) > 0:
        result = level_of(rng, extent, shards, -0.22, 0.18) * result
    return jnp.clip(result, min=-reach, max=reach).astype(kind)


def setup_inputs(seed: int = 0) -> dict:
    seeds = jax.random.split(jax.random.key(seed), 10)
    return {
        "hot_ids": set_ends(ranked_ids(seeds[0], (LOOKUPS,), HOT, 2), jax.random.fold_in(seeds[0], 3), 0, HOT - 1).astype(jnp.int32),
        "hot_grads": noise(seeds[1], (LOOKUPS, D), 1.0, 6.0, ((0, 32),)),
        "hot_rows": noise(seeds[2], (HOT, D), 1.0, 6.0, (), jnp.float32),
        "hot_accum": jnp.clip(jnp.exp(jax.random.uniform(seeds[3], (HOT,), jnp.float32, math.log(0.5), math.log(4.0))), 0.5, 4.0),
        "cold_counts": draw_cold_counts(jax.random.fold_in(seeds[9], 71), 0),
        "cold_slots": set_ends(jax.random.randint(seeds[5], (OWNERS, OWNERS, CAP), 0, COLD_DEV), jax.random.fold_in(seeds[5], 1), 0, COLD_DEV - 1).astype(jnp.int32),
        "cold_grads": noise(seeds[6], (OWNERS, OWNERS, CAP, D), 1.0, 6.0, ((0, 32),)),
        "cold_rows": noise(seeds[7], (COLD, D), 1.0, 6.0, ((0, 32),), jnp.float32),
        "cold_accum": jnp.clip(jnp.exp(math.log(4.0) - 2.0794415 * jax.random.uniform(seeds[8], (COLD,), jnp.float32) ** level_of(seeds[8], (COLD,), ((0, 32),), -0.2, 0.2)), 0.5, 4.0),
    }


learn_rate = 0.5

def adagrad(table_rows, accum_rows, gradient):
    accum_new = accum_rows + lax.optimization_barrier(jnp.mean(gradient * gradient, axis=1))
    return (table_rows - learn_rate * gradient / jnp.sqrt(accum_new)[:, None], accum_new)

def reference(hot_ids, hot_grads, hot_rows, hot_accum, cold_counts, cold_slots, cold_grads, cold_rows, cold_accum):
    hot_sum = jax.ops.segment_sum(hot_grads.astype(jnp.float32), hot_ids, num_segments=HOT)
    new_hot_rows, new_hot_accum = adagrad(hot_rows, hot_accum, hot_sum)
    slot_index = jnp.arange(CAP, dtype=jnp.int32)
    live_mask = slot_index[None, None, :] < cold_counts[:, :, None]
    owners_col = jnp.arange(OWNERS, dtype=jnp.int32)[None, :, None]
    target = (owners_col * COLD_DEV + cold_slots).astype(jnp.int32)
    masked_terms = jnp.where(live_mask[..., None], cold_grads.astype(jnp.float32), 0.0)
    cold_sum = jax.ops.segment_sum(masked_terms.reshape(-1, D), target.reshape(-1), num_segments=COLD)
    new_cold_rows, new_cold_accum = adagrad(cold_rows, cold_accum, cold_sum)
    return (new_hot_rows, new_hot_accum, new_cold_rows, new_cold_accum)
```

```python
import functools

import jax
import jax.numpy as jnp
from jax import lax
from jax.experimental import pallas as pl
from jax.experimental.pallas import tpu as pltpu
from jax.sharding import PartitionSpec as P

learn_rate = 0.5
LANES = 128
PAD = 8
BOTH = ("rep", "shard")


def adagrad(rows, accum_row, grad):
    m = rows.shape[0]
    diag = lax.broadcasted_iota(jnp.int32, (m, LANES), 0) == lax.broadcasted_iota(
        jnp.int32, (m, LANES), 1
    )
    square = jnp.sum(grad * grad, axis=1, keepdims=True) * (1.0 / grad.shape[1])
    accum = jnp.sum(jnp.where(diag, accum_row, 0.0), axis=1, keepdims=True)
    accum_new = accum + square
    rows_new = rows - grad * (learn_rate / jnp.sqrt(accum_new))
    accum_new_row = jnp.sum(jnp.where(diag, accum_new, 0.0), axis=0, keepdims=True)
    return rows_new, accum_new_row


def onehot_dot(ids, base, rows, grads):
    lookups = ids.shape[1]
    row = lax.broadcasted_iota(jnp.int32, (rows, lookups), 0)
    hit = jnp.where(row == ids - base, 1.0, 0.0).astype(jnp.bfloat16)
    return jnp.dot(hit, grads, preferred_element_type=jnp.float32)


def kernel(
    reps, shards,
    ids, grads, hot_rows, hot_accum, cold_ids, cold_grads, cold_rows, cold_accum,
    hot_out, cold_out, cold_accum_out,
    ids_buf, grads_buf, acc, z_buf, rows_buf, cold_buf, cids_buf, cgrads_buf,
    raw_send, raw_recv, raw_core_send, raw_core_recv, z_send, z_recv,
    zg_send, zg_recv, rg_send, rg_recv, core_send, core_recv,
    cold_send, cold_recv, local_sem,
):
    total = reps * shards
    depth = shards // 2
    bits = reps.bit_length() - 1
    own_rows = acc.shape[1]
    half_rows = own_rows // 2
    rep, shard = lax.axis_index("rep"), lax.axis_index("shard")
    z, core = shard // 2, shard % 2
    me = rep * shards + shard
    partner = {"rep": rep, "shard": z * 2 + 1 - core}

    def flip(r, bit):
        m = 1 << bit
        return r + m * (1 - 2 * ((r // m) % 2))

    orders = (tuple(range(bits)), tuple(reversed(range(bits))))

    def origin(h, i):
        r = rep
        for k in range(bits):
            if (i >> k) & 1:
                r = flip(r, orders[h][k])
        return r

    def remote(src, dst, s_sem, r_sem, device):
        return pltpu.make_async_remote_copy(
            src_ref=src, dst_ref=dst, send_sem=s_sem, recv_sem=r_sem,
            device_id=device, device_id_type=pl.DeviceIdType.MESH,
        )

    chunk = (core * reps + rep) * depth + z
    loads = [
        pltpu.make_async_copy(cold_rows, cold_buf, local_sem.at[0]),
        pltpu.make_async_copy(hot_rows.at[pl.ds(2 * chunk, 2)], rows_buf, local_sem.at[1]),
        pltpu.make_async_copy(cold_ids.at[me], cids_buf.at[me], local_sem.at[2]),
        pltpu.make_async_copy(cold_grads.at[me], cgrads_buf.at[me], local_sem.at[3]),
    ]
    for copy in loads:
        copy.start()

    barrier = pltpu.get_barrier_semaphore()

    @pl.loop(1, total)
    def _(d):
        p = (me + d) % total
        pl.semaphore_signal(
            barrier, inc=1, device_id={"rep": p // shards, "shard": p % shards},
            device_id_type=pl.DeviceIdType.MESH,
        )

    pl.semaphore_wait(barrier, total - 1)

    sends = []
    arrivals = {}

    def raw_ref(h, i):
        if i == 0:
            return ids.at[h], grads.at[h]
        return ids_buf.at[0, h, i], grads_buf.at[0, h, i]

    def top(i):
        return i.bit_length() - 1

    def relay(h, i, q):
        j = i | (1 << q)
        device = {"rep": flip(rep, orders[h][q]), "shard": shard}
        pair = []
        for k, (src, buf) in enumerate(zip(raw_ref(h, i), (ids_buf, grads_buf))):
            slot = (h * reps + j) * 2 + k
            pair.append(remote(src, buf.at[0, h, j], raw_send.at[slot], raw_recv.at[slot], device))
        for copy in pair:
            copy.start()
            sends.append(copy)
        arrivals[h, j] = pair

    core_pairs = {}

    def cross(h, i):
        pair = []
        for k, (src, buf) in enumerate(zip(raw_ref(h, i), (ids_buf, grads_buf))):
            slot = (h * reps + i) * 2 + k
            pair.append(
                remote(src, buf.at[1, h, i], raw_core_send.at[slot], raw_core_recv.at[slot], partner)
            )
        for copy in pair:
            copy.start()
            sends.append(copy)
        core_pairs[h, i] = pair

    for q in range(bits):
        for h in range(2):
            relay(h, 0, q)
    for h in range(2):
        cross(h, 0)

    @pl.loop(1, total)
    def _(d):
        p = (me + d) % total
        device = {"rep": p // shards, "shard": p % shards}
        remote(cold_ids.at[p], cids_buf.at[me], cold_send.at[0], cold_recv.at[0], device).start()
        remote(cold_grads.at[p], cgrads_buf.at[me], cold_send.at[1], cold_recv.at[1], device).start()

    share = (core * reps + rep) * depth

    def block_sum(c, i, base):
        value = None
        for h in range(2):
            ids_ref, grads_ref = raw_ref(h, i) if c == 0 else (ids_buf.at[1, h, i], grads_buf.at[1, h, i])
            part = onehot_dot(ids_ref[...], base, own_rows, grads_ref[...])
            value = part if value is None else value + part
        return value

    def z_copy(d, zc):
        target = {"rep": rep, "shard": zc * 2 + core}
        return remote(acc.at[zc], z_buf.at[d - 1], z_send.at[d - 1], z_recv.at[d - 1], target)

    for i in range(reps):
        if i > 0:
            for h in range(2):
                for copy in arrivals[h, i]:
                    copy.wait_recv()
                for q in range(top(i) + 1, bits):
                    relay(h, i, q)
                cross(h, i)
        for c in range(2):
            if c == 1:
                for h in range(2):
                    for copy in core_pairs[h, i]:
                        copy.wait_recv()
            last = i == reps - 1 and c == 1

            @pl.loop(1, depth + 1)
            def _(d):
                zc = (z + d) % depth
                value = block_sum(c, i, (share + zc) * own_rows)
                if i == 0 and c == 0:
                    acc[zc] = value
                else:
                    acc[zc] += value
                if last:
                    @pl.when(d >= 2)
                    def _():
                        z_copy(d - 1, (z + d - 1) % depth).start()

    for copy in loads:
        copy.wait()
    for k, buf in enumerate((cids_buf, cgrads_buf)):
        part = buf.at[pl.ds(0, total - 1)]
        pltpu.make_async_copy(part, part, cold_recv.at[k]).wait()
    capacity = cgrads_buf.shape[1]
    group = LANES // capacity
    cold_id_row = jnp.concatenate(
        [jnp.sum(cids_buf[g * group:(g + 1) * group], axis=0) for g in range(total // group)], axis=1
    ) - 1

    step_rows = 2 * LANES

    @pl.loop(0, cold_buf.shape[0] // step_rows)
    def _(b):
        terms = cgrads_buf[...].reshape(total * capacity, LANES)
        grad = onehot_dot(cold_id_row, b * step_rows, step_rows, terms)
        for s in range(2):
            at = pl.ds(pl.multiple_of(b * step_rows + s * LANES, LANES), LANES)
            new_rows, new_accum = adagrad(
                cold_buf[at], cold_accum[2 * b + s], grad[s * LANES:(s + 1) * LANES]
            )
            cold_out[at] = new_rows
            cold_accum_out[2 * b + s] = new_accum

    @pl.loop(1, depth)
    def _(d):
        z_copy(d, (z + d) % depth).wait_recv()

    for h in range(2):
        at = pl.ds(h * half_rows, half_rows)
        grad = acc[z, at]
        for d in range(1, depth):
            grad += z_buf[d - 1, at]
        new_rows, new_accum = adagrad(rows_buf[h], hot_accum[2 * chunk + h], grad)
        hot_out[2 * chunk + h, pl.ds(0, half_rows)] = new_rows
        hot_out[2 * chunk + h, pl.ds(half_rows, PAD)] = jnp.broadcast_to(new_accum, (PAD, LANES))

    def zg_copy(d):
        target = {"rep": rep, "shard": ((z + d) % depth) * 2 + core}
        part = hot_out.at[pl.ds(2 * chunk, 2)]
        return remote(part, part, zg_send.at[d - 1], zg_recv.at[d - 1], target)

    for d in range(1, depth):
        zg_copy(d).start()

    gathered = {}

    def out_block(d, h, i):
        zc = (z + depth - d) % depth
        return hot_out.at[2 * ((core * reps + origin(h, i)) * depth + zc) + h]

    def spread(d, h, i):
        part = out_block(d, h, i)
        for q in range(top(i) + 1, bits):
            j = i | (1 << q)
            slot = (d * 2 + h) * reps + j
            device = {"rep": flip(rep, orders[h][q]), "shard": shard}
            copy = remote(part, part, rg_send.at[slot], rg_recv.at[slot], device)
            copy.start()
            sends.append(copy)
            gathered[d, h, j] = copy
        remote(part, part, core_send.at[0], core_recv.at[0], partner).start()

    def finish(d):
        for i in range(1, reps):
            for h in range(2):
                part = out_block(d, h, i)
                slot = (d * 2 + h) * reps + i
                remote(part, part, rg_send.at[slot], rg_recv.at[slot], partner).wait_recv()
                spread(d, h, i)

    for d in range(depth):
        if d > 0:
            zg_copy(d).wait_recv()
        for h in range(2):
            spread(d, h, 0)
        if d > 0:
            finish(d - 1)
    finish(depth - 1)

    for copy in sends:
        copy.wait_send()
    for d in range(1, depth):
        z_copy(d, (z + d) % depth).wait_send()
        zg_copy(d).wait_send()
    for k, buf in enumerate((cold_ids, cold_grads)):
        part = buf.at[pl.ds(0, total - 1)]
        pltpu.make_async_copy(part, part, cold_send.at[k]).wait()
    side = reps * depth * 2
    mine = hot_out.at[pl.ds(core * side, side)]
    other = hot_out.at[pl.ds((1 - core) * side, side)]
    pltpu.make_async_copy(mine, mine, core_send.at[0]).wait()
    pltpu.make_async_copy(other, other, core_recv.at[0]).wait()


def local(
    hot_ids, hot_grads, hot_rows, hot_accum, cold_counts, cold_slots, cold_grads, cold_rows, cold_accum
):
    reps, shards = lax.axis_size("rep"), lax.axis_size("shard")
    total, depth = reps * shards, shards // 2
    assert reps & (reps - 1) == 0 and shards % 2 == 0
    hot_count, width = hot_rows.shape
    lookups = hot_ids.shape[0]
    own_rows = hot_count // total
    half_rows = own_rows // 2
    cold_count = cold_rows.shape[0]
    capacity = cold_slots.shape[2]
    assert width == LANES and half_rows <= LANES and LANES % capacity == 0

    half = lookups // 2
    accum_blocks = hot_accum.reshape(2 * total, 1, half_rows)
    if half_rows < LANES:
        accum_blocks = jnp.pad(accum_blocks, ((0, 0), (0, 0), (0, LANES - half_rows)))
    group = LANES // capacity
    me = lax.axis_index("rep") * shards + lax.axis_index("shard")
    lane = lax.broadcasted_iota(jnp.int32, (total, 1, LANES), 2)
    live = (lane // capacity == me % group) & (lane % capacity < cold_counts.reshape(total, 1, 1))
    slot_lanes = jnp.tile(cold_slots.reshape(total, 1, capacity), (1, 1, group))
    cold_ids = jnp.where(live, slot_lanes + 1, 0)

    f32, i32, bf16 = jnp.float32, jnp.int32, jnp.bfloat16
    vmem, anywhere = pl.BlockSpec(memory_space=pltpu.VMEM), pl.BlockSpec(memory_space=pl.ANY)
    dma = pltpu.SemaphoreType.DMA
    hot_out, cold_out, cold_accum_out = pl.pallas_call(
        functools.partial(kernel, reps, shards),
        out_shape=(
            jax.ShapeDtypeStruct((2 * total, half_rows + PAD, LANES), f32),
            jax.ShapeDtypeStruct((cold_count, LANES), f32),
            jax.ShapeDtypeStruct((cold_count // LANES, 1, LANES), f32),
        ),
        in_specs=[vmem, vmem, anywhere, vmem, vmem, vmem, anywhere, vmem],
        out_specs=(vmem, vmem, vmem),
        scratch_shapes=[
            pltpu.VMEM((2, 2, reps, 1, half), i32),
            pltpu.VMEM((2, 2, reps, half, LANES), bf16),
            pltpu.VMEM((depth, own_rows, LANES), f32),
            pltpu.VMEM((max(depth - 1, 1), own_rows, LANES), f32),
            pltpu.VMEM((2, half_rows, LANES), f32),
            pltpu.VMEM((cold_count, LANES), f32),
            pltpu.VMEM((total, 1, LANES), i32),
            pltpu.VMEM((total, capacity, LANES), bf16),
            dma((4 * reps,)), dma((4 * reps,)), dma((4 * reps,)), dma((4 * reps,)),
            dma((depth,)), dma((depth,)), dma((depth,)), dma((depth,)),
            dma((2 * depth * reps,)), dma((2 * depth * reps,)),
            dma((1,)), dma((1,)), dma((2,)), dma((2,)), dma((4,)),
        ],
        compiler_params=pltpu.CompilerParams(collective_id=0, has_side_effects=True),
    )(
        hot_ids.reshape(2, 1, half),
        hot_grads.reshape(2, half, LANES),
        hot_rows.reshape(2 * total, half_rows, LANES),
        accum_blocks,
        cold_ids,
        cold_grads.reshape(total, capacity, LANES),
        cold_rows,
        cold_accum.reshape(cold_count // LANES, 1, LANES),
    )
    return (
        hot_out[:, :half_rows].reshape(hot_count, LANES),
        hot_out[:, half_rows, :half_rows].reshape(hot_count),
        cold_out,
        cold_accum_out.reshape(cold_count),
    )


def solution(mesh):
    placed = (
        P(BOTH), P(BOTH, None), P(), P(), P(BOTH, None), P(BOTH, None, None),
        P(BOTH, None, None, None), P(BOTH, None), P(BOTH),
    )
    return jax.shard_map(
        local,
        mesh=mesh,
        in_specs=placed,
        out_specs=(P(), P(), P(BOTH, None), P(BOTH)),
        check_vma=False,
    )
```

```python
import functools

import jax
import jax.numpy as jnp
from jax import lax
from jax.experimental import pallas as pl
from jax.experimental.pallas import tpu as pltpu
from jax.sharding import PartitionSpec as P

learn_rate = 0.5
LANES = 128
PAD = 8
BOTH = ("rep", "shard")


def adagrad(rows, accum_row, grad):
    m = rows.shape[0]
    diag = lax.broadcasted_iota(jnp.int32, (m, LANES), 0) == lax.broadcasted_iota(
        jnp.int32, (m, LANES), 1
    )
    square = jnp.sum(grad * grad, axis=1, keepdims=True) * (1.0 / grad.shape[1])
    accum = jnp.sum(jnp.where(diag, accum_row, 0.0), axis=1, keepdims=True)
    accum_new = accum + square
    rows_new = rows - grad * (learn_rate / jnp.sqrt(accum_new))
    accum_new_row = jnp.sum(jnp.where(diag, accum_new, 0.0), axis=0, keepdims=True)
    return rows_new, accum_new_row


def onehot_dot(ids, base, rows, grads):
    lookups = ids.shape[1]
    row = lax.broadcasted_iota(jnp.int32, (rows, lookups), 0)
    hit = jnp.where(row == ids - base, 1.0, 0.0).astype(jnp.bfloat16)
    return jnp.dot(hit, grads, preferred_element_type=jnp.float32)


def kernel(
    reps, shards,
    ids, grads, hot_rows, hot_accum, cold_ids, cold_grads, cold_rows, cold_accum,
    hot_out, hot_accum_out, cold_out, cold_accum_out,
    hot_buf, ids_buf, grads_buf, acc, z_buf, rows_buf, cold_buf, cids_buf, cgrads_buf,
    raw_send, raw_recv, raw_core_send, raw_core_recv, z_send, z_recv,
    zg_send, zg_recv, rg_send, rg_recv, core_send, core_recv,
    cold_send, cold_recv, local_sem, out_sem,
):
    total = reps * shards
    depth = shards // 2
    bits = reps.bit_length() - 1
    own_rows = acc.shape[1]
    half_rows = own_rows // 2
    rep, shard = lax.axis_index("rep"), lax.axis_index("shard")
    z, core = shard // 2, shard % 2
    me = rep * shards + shard
    partner = {"rep": rep, "shard": z * 2 + 1 - core}

    def flip(r, bit):
        m = 1 << bit
        return r + m * (1 - 2 * ((r // m) % 2))

    def across(d):
        r = 0
        for k in range(depth.bit_length() - 1):
            r += (1 << k) * ((z // (1 << k) + d // (1 << k)) % 2)
        return r

    orders = (tuple(range(bits)), tuple(reversed(range(bits))))

    def origin(h, i):
        r = rep
        for k in range(bits):
            if (i >> k) & 1:
                r = flip(r, orders[h][k])
        return r

    def remote(src, dst, s_sem, r_sem, device):
        return pltpu.make_async_remote_copy(
            src_ref=src, dst_ref=dst, send_sem=s_sem, recv_sem=r_sem,
            device_id=device, device_id_type=pl.DeviceIdType.MESH,
        )

    chunk = (core * reps + rep) * depth + z
    loads = [
        pltpu.make_async_copy(cold_rows, cold_buf, local_sem.at[0]),
        pltpu.make_async_copy(hot_rows.at[pl.ds(2 * chunk, 2)], rows_buf, local_sem.at[1]),
        pltpu.make_async_copy(cold_ids.at[me], cids_buf.at[me], local_sem.at[2]),
        pltpu.make_async_copy(cold_grads.at[me], cgrads_buf.at[me], local_sem.at[3]),
    ]
    for copy in loads:
        copy.start()

    barrier = pltpu.get_barrier_semaphore()

    @pl.loop(1, total)
    def _(d):
        p = (me + d) % total
        pl.semaphore_signal(
            barrier, inc=1, device_id={"rep": p // shards, "shard": p % shards},
            device_id_type=pl.DeviceIdType.MESH,
        )

    pl.semaphore_wait(barrier, total - 1)

    sends = []
    arrivals = {}

    def raw_ref(h, i):
        if i == 0:
            return ids.at[h], grads.at[h]
        return ids_buf.at[0, h, i], grads_buf.at[0, h, i]

    def top(i):
        return i.bit_length() - 1

    def relay(h, i, q):
        j = i | (1 << q)
        device = {"rep": flip(rep, orders[h][q]), "shard": shard}
        pair = []
        for k, (src, buf) in enumerate(zip(raw_ref(h, i), (ids_buf, grads_buf))):
            slot = (h * reps + j) * 2 + k
            pair.append(remote(src, buf.at[0, h, j], raw_send.at[slot], raw_recv.at[slot], device))
        for copy in pair:
            copy.start()
            sends.append(copy)
        arrivals[h, j] = pair

    core_pairs = {}

    def cross(h, i):
        pair = []
        for k, (src, buf) in enumerate(zip(raw_ref(h, i), (ids_buf, grads_buf))):
            slot = (h * reps + i) * 2 + k
            pair.append(
                remote(src, buf.at[1, h, i], raw_core_send.at[slot], raw_core_recv.at[slot], partner)
            )
        for copy in pair:
            copy.start()
            sends.append(copy)
        core_pairs[h, i] = pair

    for q in range(bits):
        for h in range(2):
            relay(h, 0, q)
    for h in range(2):
        cross(h, 0)

    @pl.loop(1, total)
    def _(d):
        p = (me + d) % total
        device = {"rep": p // shards, "shard": p % shards}
        remote(cold_ids.at[p], cids_buf.at[me], cold_send.at[0], cold_recv.at[0], device).start()
        remote(cold_grads.at[p], cgrads_buf.at[me], cold_send.at[1], cold_recv.at[1], device).start()

    share = (core * reps + rep) * depth

    def block_sum(c, i, base):
        value = None
        for h in range(2):
            ids_ref, grads_ref = raw_ref(h, i) if c == 0 else (ids_buf.at[1, h, i], grads_buf.at[1, h, i])
            part = onehot_dot(ids_ref[...], base, own_rows, grads_ref[...])
            value = part if value is None else value + part
        return value

    def z_copy(d, zc):
        target = {"rep": rep, "shard": zc * 2 + core}
        return remote(acc.at[zc], z_buf.at[d - 1], z_send.at[d - 1], z_recv.at[d - 1], target)

    for i in range(reps):
        if i > 0:
            for h in range(2):
                for copy in arrivals[h, i]:
                    copy.wait_recv()
                for q in range(top(i) + 1, bits):
                    relay(h, i, q)
                cross(h, i)
        for c in range(2):
            if c == 1:
                for h in range(2):
                    for copy in core_pairs[h, i]:
                        copy.wait_recv()
            last = i == reps - 1 and c == 1

            @pl.loop(1, depth + 1)
            def _(d):
                zc = across(d % depth)
                value = block_sum(c, i, (share + zc) * own_rows)
                if i == 0 and c == 0:
                    acc[zc] = value
                else:
                    acc[zc] += value
                if last:
                    @pl.when(d >= 2)
                    def _():
                        z_copy(d - 1, across(d - 1)).start()

    for copy in loads:
        copy.wait()
    for k, buf in enumerate((cids_buf, cgrads_buf)):
        part = buf.at[pl.ds(0, total - 1)]
        pltpu.make_async_copy(part, part, cold_recv.at[k]).wait()
    capacity = cgrads_buf.shape[1]
    group = LANES // capacity
    cold_id_row = jnp.concatenate(
        [jnp.sum(cids_buf[g * group:(g + 1) * group], axis=0) for g in range(total // group)], axis=1
    ) - 1

    step_rows = 2 * LANES

    @pl.loop(0, cold_buf.shape[0] // step_rows)
    def _(b):
        terms = cgrads_buf[...].reshape(total * capacity, LANES)
        grad = onehot_dot(cold_id_row, b * step_rows, step_rows, terms)
        for s in range(2):
            at = pl.ds(pl.multiple_of(b * step_rows + s * LANES, LANES), LANES)
            new_rows, new_accum = adagrad(
                cold_buf[at], cold_accum[2 * b + s], grad[s * LANES:(s + 1) * LANES]
            )
            cold_buf[at] = new_rows
            cold_accum_out[2 * b + s] = new_accum

    cold_copy = pltpu.make_async_copy(cold_buf, cold_out, out_sem.at[0])
    cold_copy.start()

    @pl.loop(1, depth)
    def _(d):
        z_copy(d, across(d)).wait_recv()

    for h in range(2):
        at = pl.ds(h * half_rows, half_rows)
        grad = acc[z, at]
        for d in range(1, depth):
            grad += z_buf[d - 1, at]
        new_rows, new_accum = adagrad(rows_buf[h], hot_accum[2 * chunk + h], grad)
        hot_buf[2 * chunk + h, pl.ds(0, half_rows)] = new_rows
        hot_buf[2 * chunk + h, pl.ds(half_rows, PAD)] = jnp.broadcast_to(new_accum, (PAD, LANES))

    def zg_copy(d):
        target = {"rep": rep, "shard": across(d) * 2 + core}
        part = hot_buf.at[pl.ds(2 * chunk, 2)]
        return remote(part, part, zg_send.at[d - 1], zg_recv.at[d - 1], target)

    for d in range(1, depth):
        zg_copy(d).start()

    gathered = {}

    def out_block(d, h, i, side_of=core):
        zc = across(d)
        return 2 * ((side_of * reps + origin(h, i)) * depth + zc) + h

    def publish(block):
        pltpu.make_async_copy(
            hot_buf.at[block, pl.ds(0, half_rows)], hot_out.at[block], out_sem.at[1]
        ).start()

    def spread(d, h, i):
        part = hot_buf.at[out_block(d, h, i)]
        for q in range(top(i) + 1, bits):
            j = i | (1 << q)
            slot = (d * 2 + h) * reps + j
            device = {"rep": flip(rep, orders[h][q]), "shard": shard}
            copy = remote(part, part, rg_send.at[slot], rg_recv.at[slot], device)
            copy.start()
            sends.append(copy)
            gathered[d, h, j] = copy
        slot = (d * 2 + h) * reps + i
        copy = remote(part, part, core_send.at[slot], core_recv.at[slot], partner)
        copy.start()
        sends.append(copy)
        publish(out_block(d, h, i))

    def finish(d):
        for i in range(1, reps):
            for h in range(2):
                part = hot_buf.at[out_block(d, h, i)]
                slot = (d * 2 + h) * reps + i
                remote(part, part, rg_send.at[slot], rg_recv.at[slot], partner).wait_recv()
                spread(d, h, i)

    def crossed(d):
        for i in range(reps):
            for h in range(2):
                block = out_block(d, h, i, 1 - core)
                part = hot_buf.at[block]
                slot = (d * 2 + h) * reps + i
                remote(part, part, core_send.at[slot], core_recv.at[slot], partner).wait_recv()
                publish(block)

    for d in range(depth):
        if d > 0:
            zg_copy(d).wait_recv()
        for h in range(2):
            spread(d, h, 0)
        if d > 0:
            finish(d - 1)
        if d > 1:
            crossed(d - 2)
    finish(depth - 1)
    for d in range(max(depth - 2, 0), depth):
        crossed(d)

    @pl.loop(0, 2 * total)
    def _(b):
        hot_accum_out[b] = hot_buf[b, pl.ds(half_rows, 1)]

    for copy in sends:
        copy.wait_send()
    for d in range(1, depth):
        z_copy(d, across(d)).wait_send()
        zg_copy(d).wait_send()
    for k, buf in enumerate((cold_ids, cold_grads)):
        part = buf.at[pl.ds(0, total - 1)]
        pltpu.make_async_copy(part, part, cold_send.at[k]).wait()
    cold_copy.wait()
    pltpu.make_async_copy(hot_out, hot_out, out_sem.at[1]).wait()


def local(
    hot_ids, hot_grads, hot_rows, hot_accum, cold_counts, cold_slots, cold_grads, cold_rows, cold_accum
):
    reps, shards = lax.axis_size("rep"), lax.axis_size("shard")
    total, depth = reps * shards, shards // 2
    assert reps & (reps - 1) == 0 and shards & (shards - 1) == 0
    hot_count, width = hot_rows.shape
    lookups = hot_ids.shape[0]
    own_rows = hot_count // total
    half_rows = own_rows // 2
    cold_count = cold_rows.shape[0]
    capacity = cold_slots.shape[2]
    assert width == LANES and half_rows <= LANES and LANES % capacity == 0

    half = lookups // 2
    accum_blocks = hot_accum.reshape(2 * total, 1, half_rows)
    if half_rows < LANES:
        accum_blocks = jnp.pad(accum_blocks, ((0, 0), (0, 0), (0, LANES - half_rows)))
    group = LANES // capacity
    me = lax.axis_index("rep") * shards + lax.axis_index("shard")
    lane = lax.broadcasted_iota(jnp.int32, (total, 1, LANES), 2)
    live = (lane // capacity == me % group) & (lane % capacity < cold_counts.reshape(total, 1, 1))
    slot_lanes = jnp.tile(cold_slots.reshape(total, 1, capacity), (1, 1, group))
    cold_ids = jnp.where(live, slot_lanes + 1, 0)

    f32, i32, bf16 = jnp.float32, jnp.int32, jnp.bfloat16
    vmem, anywhere = pl.BlockSpec(memory_space=pltpu.VMEM), pl.BlockSpec(memory_space=pl.ANY)
    dma = pltpu.SemaphoreType.DMA
    hot_out, hot_accum_out, cold_out, cold_accum_out = pl.pallas_call(
        functools.partial(kernel, reps, shards),
        out_shape=(
            jax.ShapeDtypeStruct((2 * total, half_rows, LANES), f32),
            jax.ShapeDtypeStruct((2 * total, 1, LANES), f32),
            jax.ShapeDtypeStruct((cold_count, LANES), f32),
            jax.ShapeDtypeStruct((cold_count // LANES, 1, LANES), f32),
        ),
        in_specs=[vmem, vmem, anywhere, vmem, vmem, vmem, anywhere, vmem],
        out_specs=(anywhere, vmem, anywhere, vmem),
        scratch_shapes=[
            pltpu.VMEM((2 * total, half_rows + PAD, LANES), f32),
            pltpu.VMEM((2, 2, reps, 1, half), i32),
            pltpu.VMEM((2, 2, reps, half, LANES), bf16),
            pltpu.VMEM((depth, own_rows, LANES), f32),
            pltpu.VMEM((max(depth - 1, 1), own_rows, LANES), f32),
            pltpu.VMEM((2, half_rows, LANES), f32),
            pltpu.VMEM((cold_count, LANES), f32),
            pltpu.VMEM((total, 1, LANES), i32),
            pltpu.VMEM((total, capacity, LANES), bf16),
            dma((4 * reps,)), dma((4 * reps,)), dma((4 * reps,)), dma((4 * reps,)),
            dma((depth,)), dma((depth,)), dma((depth,)), dma((depth,)),
            dma((2 * depth * reps,)), dma((2 * depth * reps,)),
            dma((2 * depth * reps,)), dma((2 * depth * reps,)),
            dma((2,)), dma((2,)), dma((4,)), dma((2,)),
        ],
        compiler_params=pltpu.CompilerParams(collective_id=0, has_side_effects=True),
    )(
        hot_ids.reshape(2, 1, half),
        hot_grads.reshape(2, half, LANES),
        hot_rows.reshape(2 * total, half_rows, LANES),
        accum_blocks,
        cold_ids,
        cold_grads.reshape(total, capacity, LANES),
        cold_rows,
        cold_accum.reshape(cold_count // LANES, 1, LANES),
    )
    return (
        hot_out.reshape(hot_count, LANES),
        hot_accum_out[:, 0, :half_rows].reshape(hot_count),
        cold_out,
        cold_accum_out.reshape(cold_count),
    )


def solution(mesh):
    placed = (
        P(BOTH), P(BOTH, None), P(), P(), P(BOTH, None), P(BOTH, None, None),
        P(BOTH, None, None, None), P(BOTH, None), P(BOTH),
    )
    return jax.shard_map(
        local,
        mesh=mesh,
        in_specs=placed,
        out_specs=(P(), P(), P(BOTH, None), P(BOTH)),
        check_vma=False,
    )
```
